16 devices in a mesh: ep: 16 (over z, y, x, core).
Axes of the slice: x: 2, y: 2, z: 2, core: 2. Of those that a mesh axis runs over, the one named last changes fastest.
Arguments:
- tokens: bfloat16 [256, 256, 1024], P('ep')
- pad_mask: int32 [256, 256], P('ep')
- second_draw: float32 [256, 256], P('ep')
- choices: int32 [256, 256, 2], P('ep')
- norm_attn: float32 [1024], replicated
- w_query: bfloat16 [1024, 16, 64], replicated
- w_key: bfloat16 [1024, 16, 64], replicated
- w_value: bfloat16 [1024, 16, 64], replicated
- w_attn_out: bfloat16 [16, 64, 1024], replicated
- norm_moe: float32 [1024], replicated
- w_gate: float32 [1024, 32], replicated
- w_in: bfloat16 [32, 1024, 2816], P('ep')
- w_out: bfloat16 [32, 2816, 1024], P('ep')
Outputs:
- output 1: bfloat16 [256, 256, 1024], P('ep')
- output 2: float32 [], replicated
All inputs are finite; a program needn't handle non-finite values.
Results may differ from the reference program's by a relative error of at most 0.02.
Values are sent between devices in bfloat16 or wider.
A program may use at most 1 GiB of HBM per device.

```python
import math
import jax
import jax.numpy as jnp
from jax import lax

D_MODEL = 1024
NUM_HEADS = 16
HEAD_DIM = 64
FF_DIM = 2816
EXPERTS = 32
GROUPS = 256
SEQ_LEN = 256

CAPACITY = (2 * SEQ_LEN + EXPERTS - 1) // EXPERTS
NORM_EPS = 1e-6


def rms_norm(values, scale_vec):
    values_f = values.astype(jnp.float32)
    inv_rms = lax.rsqrt(jnp.mean(values_f * values_f, axis=-1, keepdims=True) + NORM_EPS)
    return (values_f * inv_rms * scale_vec).astype(jnp.bfloat16)


def draw_routing(base_key):
    key_list = jax.random.split(base_key, 7)
    lengths = jax.random.randint(key_list[0], (GROUPS,), SEQ_LEN // 2, SEQ_LEN + 1)
    lengths = lengths.at[0].set(SEQ_LEN).at[1].set(SEQ_LEN // 2)
    pad_mask = (jnp.arange(SEQ_LEN)[None, :] < lengths[:, None]).astype(jnp.int32)
    second_draw = jax.random.uniform(key_list[1], (GROUPS, SEQ_LEN), jnp.float32)
    hot_expert = jax.random.randint(key_list[2], (GROUPS, 1), 0, EXPERTS)
    hot_share = jax.random.randint(key_list[3], (GROUPS, 1), 0, 5)
    coin_draw = jax.random.randint(key_list[4], (GROUPS, SEQ_LEN), 0, 16)
    any_first = jax.random.randint(key_list[5], (GROUPS, SEQ_LEN), 0, EXPERTS)
    first_pick = jnp.where(coin_draw < hot_share, hot_expert, any_first)
    offset = jax.random.randint(key_list[6], (GROUPS, SEQ_LEN), 1, EXPERTS)
    second_pick = (first_pick + offset) % EXPERTS
    choices = jnp.stack([first_pick, second_pick], axis=-1).astype(jnp.int32)
    return pad_mask, second_draw, choices


def setup_inputs(seed: int = 0) -> dict:
    key_list = jax.random.split(jax.random.key(seed), 11)
    head_width = NUM_HEADS * HEAD_DIM
    att_gain = math.sqrt(math.log(SEQ_LEN) / 2.0)
    out_gain = 0.5 * SEQ_LEN ** 0.25
    pad_mask, second_draw, choices = draw_routing(key_list[0])

    def normal_draw(index, shape, scale_val):
        return jax.random.normal(key_list[index], shape, jnp.float32) * scale_val

    return {
        "tokens": normal_draw(1, (GROUPS, SEQ_LEN, D_MODEL), 1.0).astype(jnp.bfloat16),
        "pad_mask": pad_mask,
        "second_draw": second_draw,
        "choices": choices,
        "norm_attn": 1.0 + normal_draw(2, (D_MODEL,), 0.3),
        "w_query": normal_draw(3, (D_MODEL, NUM_HEADS, HEAD_DIM), att_gain / math.sqrt(D_MODEL)).astype(jnp.bfloat16),
        "w_key": normal_draw(4, (D_MODEL, NUM_HEADS, HEAD_DIM), 1.0 / math.sqrt(D_MODEL)).astype(jnp.bfloat16),
        "w_value": normal_draw(5, (D_MODEL, NUM_HEADS, HEAD_DIM), 1.0 / math.sqrt(D_MODEL)).astype(jnp.bfloat16),
        "w_attn_out": normal_draw(6, (NUM_HEADS, HEAD_DIM, D_MODEL), out_gain / math.sqrt(head_width)).astype(jnp.bfloat16),
        "norm_moe": 1.0 + normal_draw(7, (D_MODEL,), 0.3),
        "w_gate": normal_draw(8, (D_MODEL, EXPERTS), 1.0 / math.sqrt(D_MODEL)),
        "w_in": normal_draw(9, (EXPERTS, D_MODEL, FF_DIM), 1.0 / math.sqrt(D_MODEL)).astype(jnp.bfloat16),
        "w_out": normal_draw(10, (EXPERTS, FF_DIM, D_MODEL), 2.0 / math.sqrt(FF_DIM)).astype(jnp.bfloat16),
    }


def reference(tokens, pad_mask, second_draw, choices, norm_attn, w_query, w_key, w_value, w_attn_out, norm_moe, w_gate, w_in, w_out):
    head_width = NUM_HEADS * HEAD_DIM
    wq_flat = w_query.reshape(D_MODEL, head_width)
    wk_flat = w_key.reshape(D_MODEL, head_width)
    wv_flat = w_value.reshape(D_MODEL, head_width)
    wo_flat = w_attn_out.reshape(head_width, D_MODEL)
    w_in_f = w_in.astype(jnp.float32)
    w_out_f = w_out.astype(jnp.float32)
    expert_ids = jnp.arange(EXPERTS)
    slot_ids = jnp.arange(CAPACITY)

    def one_group(group_args):
        x_grp, mask_grp, draw_grp, pick_grp = group_args
        normed = rms_norm(x_grp, norm_attn)
        q_heads = jnp.dot(normed, wq_flat, preferred_element_type=jnp.float32).astype(jnp.bfloat16).reshape(SEQ_LEN, NUM_HEADS, HEAD_DIM)
        k_heads = jnp.dot(normed, wk_flat, preferred_element_type=jnp.float32).astype(jnp.bfloat16).reshape(SEQ_LEN, NUM_HEADS, HEAD_DIM)
        v_heads = jnp.dot(normed, wv_flat, preferred_element_type=jnp.float32).astype(jnp.bfloat16).reshape(SEQ_LEN, NUM_HEADS, HEAD_DIM)
        scores = jnp.einsum("qhc,khc->hqk", q_heads.astype(jnp.float32), k_heads.astype(jnp.float32)) * (HEAD_DIM ** -0.5)
        scores = jnp.where(mask_grp[None, None, :] == 1, scores, -1e30)
        attn_probs = jax.nn.softmax(scores, axis=-1).astype(jnp.bfloat16)
        context = jnp.einsum("hqk,khc->qhc", attn_probs.astype(jnp.float32), v_heads.astype(jnp.float32)).astype(jnp.bfloat16)
        attn_out = jnp.dot(context.reshape(SEQ_LEN, head_width), wo_flat, preferred_element_type=jnp.float32)
        hidden = (x_grp.astype(jnp.float32) + attn_out).astype(jnp.bfloat16)
        moe_in = rms_norm(hidden, norm_moe)
        logits = jnp.dot(moe_in.astype(jnp.float32), w_gate)
        gate_probs = jax.nn.softmax(logits, axis=-1)
        is_valid = mask_grp == 1
        first_hot = pick_grp[:, 0:1] == expert_ids
        second_hot = pick_grp[:, 1:2] == expert_ids
        p_first = jnp.sum(jnp.where(first_hot, gate_probs, 0.0), axis=-1)
        p_second = jnp.sum(jnp.where(second_hot, gate_probs, 0.0), axis=-1)
        gate_first = p_first / (p_first + p_second)
        gate_second = p_second / (p_first + p_second)
        want_second = is_valid & (draw_grp < 2.0 * gate_second)
        first_take = (first_hot & is_valid[:, None]).astype(jnp.int32)
        first_pos = jnp.sum((jnp.cumsum(first_take, axis=0) - 1) * first_take, axis=-1)
        first_count = jnp.sum(first_take, axis=0)
        keep_first = is_valid & (first_pos < CAPACITY)
        second_take = (second_hot & want_second[:, None]).astype(jnp.int32)
        second_pos = jnp.sum((jnp.cumsum(second_take, axis=0) - 1 + jnp.minimum(first_count, CAPACITY)[None, :]) * second_take, axis=-1)
        keep_second = want_second & (second_pos < CAPACITY)
        first_slot = (first_pos[:, None] == slot_ids) & keep_first[:, None]
        second_slot = (second_pos[:, None] == slot_ids) & keep_second[:, None]
        first_mask = first_hot[:, :, None] & first_slot[:, None, :]
        second_mask = second_hot[:, :, None] & second_slot[:, None, :]
        dispatch = (first_mask | second_mask).astype(jnp.float32)
        combine = (jnp.where(first_mask, gate_first[:, None, None], 0.0) + jnp.where(second_mask, gate_second[:, None, None], 0.0)).astype(jnp.bfloat16)
        send_buf = jnp.einsum("sec,sd->ecd", dispatch, moe_in.astype(jnp.float32)).astype(jnp.bfloat16)
        inner_act = jnp.maximum(jnp.einsum("ecd,edf->ecf", send_buf.astype(jnp.float32), w_in_f), 0.0).astype(jnp.bfloat16)
        expert_out = jnp.einsum("ecf,efd->ecd", inner_act.astype(jnp.float32), w_out_f).astype(jnp.bfloat16)
        moe_out = jnp.einsum("sec,ecd->sd", combine.astype(jnp.float32), expert_out.astype(jnp.float32))
        out_grp = (hidden.astype(jnp.float32) + moe_out).astype(jnp.bfloat16)
        density = jnp.sum(jnp.where(is_valid[:, None], gate_probs, 0.0), axis=0) / SEQ_LEN
        aux_grp = jnp.sum(first_count.astype(jnp.float32) / SEQ_LEN * density)
        return out_grp, aux_grp

    out_tokens, aux_groups = lax.map(one_group, (tokens, pad_mask, second_draw, choices))
    aux_loss = EXPERTS * jnp.sum(aux_groups) / GROUPS
    return out_tokens, aux_loss
```

```python
import functools
import jax
import jax.numpy as jnp
from jax import lax
from jax.experimental import pallas as pl
from jax.experimental.pallas import tpu as pltpu
from jax.sharding import PartitionSpec as P

NORM_EPS = 1e-6
MESH = pl.DeviceIdType.MESH
F32 = jnp.float32
BF16 = jnp.bfloat16
LOG2E = 1.4426950408889634


def norm_rows(x, scale):
    inv = lax.rsqrt(jnp.mean(x * x, axis=-1, keepdims=True) + NORM_EPS)
    return (x * inv * scale).astype(BF16)


def dot_nt(a, b):
    return lax.dot_general(a, b, (((1,), (1,)), ((), ())), preferred_element_type=F32)


def dot_tn(a, b):
    return lax.dot_general(a, b, (((0,), (0,)), ((), ())), preferred_element_type=F32)


def peer_order(n):
    full = [2, 4, 8, 3, 5, 9, 6, 12, 10, 7, 13, 11, 14, 15, 1]
    return [k for k in full if k < n] if n == 16 else list(range(1, n))


def attend_kernel(n, heads, cap, groups, meta_ref, tok_ref, na_ref, wqkv_ref, wo_ref, nm_ref, wg_ref,
                  h_ref, aux_ref, loss_ref, recv_ref,
                  qkv_ref, ctx_ref, xs_ref, send_sem, recv_sem, own_sem):
    me = lax.axis_index("ep")
    g = pl.program_id(0)
    seq, d = tok_ref.shape[1], tok_ref.shape[2]
    experts = wg_ref.shape[0] // 3
    rows = experts * cap // n
    ks = peer_order(n)

    @pl.when(g == 0)
    def _():
        barrier = pltpu.get_barrier_semaphore()
        for k in ks:
            pl.semaphore_signal(barrier, inc=1, device_id=(me ^ k,), device_id_type=MESH)
        pl.semaphore_wait(barrier, n - 1)
        loss_ref[...] = jnp.zeros_like(loss_ref)

    @pl.when(g > 0)
    def _():
        p = g - 1
        for k in ks:
            peer = me ^ k
            pltpu.make_async_remote_copy(
                src_ref=xs_ref.at[p, pl.ds(pl.multiple_of(peer * rows, rows), rows)],
                dst_ref=recv_ref.at[me, p],
                send_sem=send_sem.at[p], recv_sem=recv_sem.at[me],
                device_id=(peer,), device_id_type=MESH).start()
        pltpu.make_async_copy(xs_ref.at[p, pl.ds(pl.multiple_of(me * rows, rows), rows)],
                              recv_ref.at[me, p], own_sem).start()

    @pl.when(g < groups)
    def _():
        a = norm_rows(tok_ref[0].astype(F32), na_ref[...])
        for c in range(3):
            qkv_ref[:, c * d:(c + 1) * d] = jnp.dot(
                a, wqkv_ref[:, c * d:(c + 1) * d], preferred_element_type=F32).astype(BF16)
        key_ok = meta_ref[0, 2:3, :] == 1.0
        low = lax.broadcasted_iota(jnp.int32, (seq, 128), 1) < 64
        factor = 0.125 * LOG2E

        def probs(q, k):
            s = jnp.where(key_ok, dot_nt(q, k), -1e30)
            e = jnp.exp2((s - jnp.max(s, axis=-1, keepdims=True)) * factor)
            return (e * (1.0 / jnp.sum(e, axis=-1, keepdims=True))).astype(BF16)

        def pair(i, carry):
            off = pl.multiple_of(i * 128, 128)
            q = qkv_ref[:, pl.ds(off, 128)]
            k = qkv_ref[:, pl.ds(pl.multiple_of(d + off, 128), 128)]
            v = qkv_ref[:, pl.ds(pl.multiple_of(2 * d + off, 128), 128)]
            zero = jnp.zeros_like(q)
            p0 = probs(jnp.where(low, q, zero), k)
            p1 = probs(jnp.where(low, zero, q), k)
            c = jnp.dot(p0, jnp.where(low, v, zero), preferred_element_type=F32)
            c += jnp.dot(p1, jnp.where(low, zero, v), preferred_element_type=F32)
            ctx_ref[:, pl.ds(off, 128)] = c.astype(BF16)
            return carry

        lax.fori_loop(0, heads // 2, pair, 0, unroll=2)
        attn = jnp.dot(ctx_ref[...], wo_ref[...], preferred_element_type=F32)
        h = (tok_ref[0].astype(F32) + attn).astype(BF16)
        h_ref[0] = h
        b = norm_rows(h.astype(F32), nm_ref[...])

        lg = dot_nt(wg_ref[...], b)
        lg = lg[:experts] + (lg[experts:2 * experts] + lg[2 * experts:])
        ex = jnp.exp(lg - jnp.max(lg, axis=0, keepdims=True))
        p = ex / jnp.sum(ex, axis=0, keepdims=True)
        c1 = meta_ref[0, 0:1, :]
        c2 = meta_ref[0, 1:2, :]
        draw = meta_ref[0, 3:4, :]
        valid = jnp.where(meta_ref[0, 2:3, :] == 1.0, 1.0, 0.0)
        ids = lax.broadcasted_iota(jnp.int32, (experts, seq), 0).astype(F32)
        hot1 = jnp.where(ids == c1, 1.0, 0.0)
        hot2 = jnp.where(ids == c2, 1.0, 0.0)
        p1 = jnp.sum(hot1 * p, axis=0, keepdims=True)
        p2 = jnp.sum(hot2 * p, axis=0, keepdims=True)
        g1 = p1 / (p1 + p2)
        g2 = p2 / (p1 + p2)
        want2 = valid * jnp.where(draw < 2.0 * g2, 1.0, 0.0)
        take1 = hot1 * valid
        take2 = hot2 * want2
        upper = jnp.where(lax.broadcasted_iota(jnp.int32, (seq, seq), 0)
                          <= lax.broadcasted_iota(jnp.int32, (seq, seq), 1), 1.0, 0.0).astype(BF16)
        cum1 = jnp.dot(take1.astype(BF16), upper, preferred_element_type=F32)
        cum2 = jnp.dot(take2.astype(BF16), upper, preferred_element_type=F32)
        count1 = jnp.sum(take1, axis=1, keepdims=True)
        pos1 = jnp.sum((cum1 - 1.0) * take1, axis=0, keepdims=True)
        pos2 = jnp.sum((cum2 - 1.0 + jnp.minimum(count1, float(cap))) * take2, axis=0, keepdims=True)
        slot1 = jnp.where((valid > 0.5) & (pos1 < float(cap)), c1 * float(cap) + pos1, -1.0)
        slot2 = jnp.where((want2 > 0.5) & (pos2 < float(cap)), c2 * float(cap) + pos2, -1.0)
        half = experts * cap // 2
        for part in range(2):
            slots = lax.broadcasted_iota(jnp.int32, (half, seq), 0).astype(F32) + float(part * half)
            pick = jnp.where((slots == slot1) | (slots == slot2), 1.0, 0.0).astype(BF16)
            xs_ref[g, part * half:(part + 1) * half, :] = jnp.dot(
                pick, b, preferred_element_type=F32).astype(BF16)
        density = jnp.sum(p * valid, axis=1, keepdims=True) * (1.0 / seq)
        part_loss = jnp.sum(count1 * (1.0 / seq) * density, axis=0, keepdims=True)
        loss_ref[...] += part_loss
        aux_ref[0] = jnp.concatenate([slot1, slot2, g1, g2, g1, g1, g1, g1], axis=0)

    @pl.when(g == groups)
    def _():
        for i in range(groups):
            block = xs_ref.at[i, pl.ds(0, (n - 1) * rows)]
            pltpu.make_async_copy(block, block, send_sem.at[i]).wait()
        for k in ks:
            block = recv_ref.at[me ^ k]
            pltpu.make_async_copy(block, block, recv_sem.at[me ^ k]).wait()
        block = recv_ref.at[me]
        pltpu.make_async_copy(block, block, own_sem).wait()


def expert_kernel(n, cap, groups, slots, aux_ref, x_ref, h_ref, loss_in, w_in_hbm, w_out_hbm,
                  out_ref, loss_ref,
                  w_in, w_out, mid_ref, z_ref, ret_ref, lbuf, w_sem, send_sem, recv_sem, lsend_sem, lrecv_sem):
    me = lax.axis_index("ep")
    r = pl.program_id(0)
    e_loc, d, ff = w_in.shape
    rows = e_loc * cap
    seq = h_ref.shape[1]
    ks = peer_order(n)

    def weight_copy(e, which):
        if which == 0:
            return pltpu.make_async_copy(w_in_hbm.at[e], w_in.at[e], w_sem.at[e, 0])
        return pltpu.make_async_copy(w_out_hbm.at[e], w_out.at[e], w_sem.at[e, 1])

    @pl.when(r == 0)
    def _():
        for e in range(e_loc):
            weight_copy(e, 0).start()
            weight_copy(e, 1).start()
        barrier = pltpu.get_barrier_semaphore()
        for k in ks:
            pl.semaphore_signal(barrier, inc=1, device_id=(me ^ k,), device_id_type=MESH)
        pl.semaphore_wait(barrier, n - 1)
        for k in ks:
            pltpu.make_async_remote_copy(
                src_ref=loss_in, dst_ref=lbuf.at[me], send_sem=lsend_sem, recv_sem=lrecv_sem,
                device_id=(me ^ k,), device_id_type=MESH).start()
        lbuf[me] = loss_in[...]

    @pl.when((r > 0) & (r <= groups))
    def _():
        p = r - 1
        for k in ks:
            peer = me ^ k
            pltpu.make_async_remote_copy(
                src_ref=z_ref.at[lax.rem(p, slots), peer],
                dst_ref=ret_ref.at[p, pl.ds(pl.multiple_of(me * rows, rows), rows)],
                send_sem=send_sem.at[lax.rem(p, slots)], recv_sem=recv_sem.at[p],
                device_id=(peer,), device_id_type=MESH).start()
        ret_ref[p, pl.ds(pl.multiple_of(me * rows, rows), rows), :] = z_ref[lax.rem(p, slots), me]

    def wait_sends(s):
        block = z_ref.at[s, pl.ds(0, n - 1)]
        pltpu.make_async_copy(block, block, send_sem.at[s]).wait()

    @pl.when(r < groups)
    def _():
        s = lax.rem(r, slots)

        @pl.when(r >= slots)
        def _():
            wait_sends(s)

        for e in range(e_loc):
            @pl.when(r == 0)
            def _():
                weight_copy(e, 0).wait()
            lhs = x_ref[:, 0, e * cap:(e + 1) * cap, :].reshape(n * cap, d)
            for c in range(2):
                cols = slice(c * (ff // 2), (c + 1) * (ff // 2))
                up = jnp.dot(lhs, w_in[e, :, cols], preferred_element_type=F32)
                mid_ref[:, cols] = jnp.maximum(up, 0.0).astype(BF16)

            @pl.when(r == 0)
            def _():
                weight_copy(e, 1).wait()
            for c in range(2):
                cols = slice(c * (d // 2), (c + 1) * (d // 2))
                down = jnp.dot(mid_ref[...], w_out[e, :, cols], preferred_element_type=F32)
                z_ref[s, :, e * cap:(e + 1) * cap, cols] = down.astype(BF16).reshape(n, cap, d // 2)

    @pl.when(r >= groups)
    def _():
        g = r - groups
        block = ret_ref.at[g, pl.ds(0, (n - 1) * rows)]
        pltpu.make_async_copy(block, block, recv_sem.at[g]).wait()
        slot1 = aux_ref[0, 0:1, :]
        slot2 = aux_ref[0, 1:2, :]
        g1 = aux_ref[0, 2:3, :]
        g2 = aux_ref[0, 3:4, :]
        ids = lax.broadcasted_iota(jnp.int32, (n * rows, seq), 0).astype(F32)
        comb = (jnp.where(ids == slot1, g1, 0.0) + jnp.where(ids == slot2, g2, 0.0)).astype(BF16)
        out_ref[0] = (h_ref[0].astype(F32) + dot_tn(comb, ret_ref[g])).astype(BF16)

    @pl.when(r == 2 * groups - 1)
    def _():
        for s in range(slots):
            wait_sends(s)
        pltpu.make_async_copy(lbuf.at[pl.ds(0, n - 1)], lbuf.at[pl.ds(0, n - 1)], lsend_sem).wait()
        pltpu.make_async_copy(lbuf.at[pl.ds(0, n - 1)], lbuf.at[pl.ds(0, n - 1)], lrecv_sem).wait()
        loss_ref[...] = jnp.sum(lbuf[...], axis=0)


def solution(mesh):
    n = mesh.shape["ep"]

    def local_step(tokens, pad_mask, second_draw, choices, norm_attn, w_query, w_key, w_value, w_attn_out, norm_moe, w_gate, w_in, w_out):
        groups, seq, d = tokens.shape
        heads = w_query.shape[1]
        experts = w_gate.shape[1]
        e_loc, _, ff = w_in.shape
        cap = (2 * seq + experts - 1) // experts
        rows = e_loc * cap
        flat = [w.reshape(d, d) for w in (w_query, w_key, w_value)]
        wqkv = jnp.concatenate(flat, axis=1)
        wo = w_attn_out.reshape(d, d)
        g_hi = lax.reduce_precision(w_gate, 8, 7)
        g_mid = lax.reduce_precision(w_gate - g_hi, 8, 7)
        g_lo = w_gate - g_hi - g_mid
        wg = jnp.concatenate([g_hi, g_mid, g_lo], axis=1).astype(BF16).T
        meta = jnp.stack([choices[:, :, 0].astype(F32), choices[:, :, 1].astype(F32),
                          pad_mask.astype(F32), second_draw] + [second_draw] * 4, axis=1)
        const = dict(pipeline_mode=pl.Buffered(1))
        last = groups - 1
        hidden, aux, loss, recv = pl.pallas_call(
            functools.partial(attend_kernel, n, heads, cap, groups),
            grid=(groups + 1,),
            out_shape=(jax.ShapeDtypeStruct((groups, seq, d), BF16),
                       jax.ShapeDtypeStruct((groups, 8, seq), F32),
                       jax.ShapeDtypeStruct((8, 128), F32),
                       jax.ShapeDtypeStruct((n, groups, rows, d), BF16)),
            in_specs=[pl.BlockSpec((1, 8, seq), lambda g: (jnp.minimum(g, last), 0, 0)),
                      pl.BlockSpec((1, seq, d), lambda g: (jnp.minimum(g, last), 0, 0)),
                      pl.BlockSpec((1, d), lambda g: (0, 0), **const),
                      pl.BlockSpec((d, 3 * d), lambda g: (0, 0), **const),
                      pl.BlockSpec((d, d), lambda g: (0, 0), **const),
                      pl.BlockSpec((1, d), lambda g: (0, 0), **const),
                      pl.BlockSpec((3 * experts, d), lambda g: (0, 0), **const)],
            out_specs=(pl.BlockSpec((1, seq, d), lambda g: (jnp.minimum(g, last), 0, 0)),
                       pl.BlockSpec((1, 8, seq), lambda g: (jnp.minimum(g, last), 0, 0)),
                       pl.BlockSpec((8, 128), lambda g: (0, 0)),
                       pl.BlockSpec(memory_space=pl.ANY)),
            scratch_shapes=[pltpu.VMEM((seq, 3 * d), BF16), pltpu.VMEM((seq, d), BF16),
                            pltpu.VMEM((groups, n * rows, d), BF16),
                            pltpu.SemaphoreType.DMA((groups,)), pltpu.SemaphoreType.DMA((n,)),
                            pltpu.SemaphoreType.DMA],
            compiler_params=pltpu.CompilerParams(collective_id=0, has_side_effects=True,
                                                 vmem_limit_bytes=60 * 2**20),
        )(meta, tokens, norm_attn.reshape(1, d), wqkv, wo, norm_moe.reshape(1, d), wg)

        slots = 6
        out, loss = pl.pallas_call(
            functools.partial(expert_kernel, n, cap, groups, slots),
            grid=(2 * groups,),
            out_shape=(jax.ShapeDtypeStruct((groups, seq, d), BF16), jax.ShapeDtypeStruct((8, 128), F32)),
            in_specs=[pl.BlockSpec((1, 8, seq), lambda r: (jnp.maximum(r - groups, 0), 0, 0)),
                      pl.BlockSpec((n, 1, rows, d), lambda r: (0, jnp.minimum(r, last), 0, 0)),
                      pl.BlockSpec((1, seq, d), lambda r: (jnp.maximum(r - groups, 0), 0, 0)),
                      pl.BlockSpec((8, 128), lambda r: (0, 0), **const),
                      pl.BlockSpec(memory_space=pl.ANY),
                      pl.BlockSpec(memory_space=pl.ANY)],
            out_specs=(pl.BlockSpec((1, seq, d), lambda r: (jnp.maximum(r - groups, 0), 0, 0)),
                       pl.BlockSpec((8, 128), lambda r: (0, 0))),
            scratch_shapes=[pltpu.VMEM((e_loc, d, ff), BF16), pltpu.VMEM((e_loc, ff, d), BF16),
                            pltpu.VMEM((n * cap, ff), BF16), pltpu.VMEM((slots, n, rows, d), BF16),
                            pltpu.VMEM((groups, n * rows, d), BF16), pltpu.VMEM((n, 8, 128), F32),
                            pltpu.SemaphoreType.DMA((e_loc, 2)), pltpu.SemaphoreType.DMA((slots,)),
                            pltpu.SemaphoreType.DMA((groups,)), pltpu.SemaphoreType.DMA, pltpu.SemaphoreType.DMA],
            compiler_params=pltpu.CompilerParams(collective_id=1, has_side_effects=True,
                                                 vmem_limit_bytes=63 * 2**20),
        )(aux, recv, hidden, loss, w_in, w_out)
        aux_loss = loss[0, 0] * experts / (groups * n)
        return out, aux_loss

    by_group = P("ep")
    replicated = P()
    in_specs = (by_group, by_group, by_group, by_group, replicated, replicated, replicated, replicated, replicated, replicated, replicated, by_group, by_group)
    return jax.shard_map(local_step, mesh=mesh, in_specs=in_specs, out_specs=(by_group, replicated), check_vma=False)
```

```python
import functools
import jax
import jax.numpy as jnp
from jax import lax
from jax.experimental import pallas as pl
from jax.experimental.pallas import tpu as pltpu
from jax.sharding import PartitionSpec as P

NORM_EPS = 1e-6
MESH = pl.DeviceIdType.MESH
F32 = jnp.float32
BF16 = jnp.bfloat16
LOG2E = 1.4426950408889634


def norm_rows(x, scale):
    inv = lax.rsqrt(jnp.mean(x * x, axis=-1, keepdims=True) + NORM_EPS)
    return (x * inv * scale).astype(BF16)


def dot_nn(a, b):
    return jnp.dot(a, b, preferred_element_type=F32)


def dot_nt(a, b):
    return lax.dot_general(a, b, (((1,), (1,)), ((), ())), preferred_element_type=F32)


def dot_tn(a, b):
    return lax.dot_general(a, b, (((0,), (0,)), ((), ())), preferred_element_type=F32)


def peer_order(n):
    full = [2, 4, 8, 3, 5, 9, 6, 12, 10, 7, 13, 11, 14, 15, 1]
    return full if n == 16 else list(range(1, n))


def layer_kernel(n, heads, cap, groups, mask_ref, draw_ref, pick_ref, tok_ref, na_ref, nm_ref, wg_ref,
                 wq_hbm, wk_hbm, wv_hbm, wo_hbm, w_in_hbm, w_out_hbm,
                 out_hbm, loss_ref, recv_hbm, ret_hbm,
                 wa_ref, wg3_ref, qkv_ref, ctx_ref, hbuf, obuf, aux_ref, lacc, lbuf, xs_ref,
                 w_in, w_out, mid_ref, lhs_ref, retb,
                 wa_sem, wf_sem, h_sem, o_sem, l_sem, r_sem, own_sem, own2_sem,
                 send_sem, recv_sem, send2_sem, recv2_sem, lsend_sem, lrecv_sem):
    me = lax.axis_index("ep")
    t = pl.program_id(0)
    seq, d = tok_ref.shape[1], tok_ref.shape[2]
    experts = wg_ref.shape[0]
    e_loc, _, ff = w_in.shape
    rows = e_loc * cap
    ks = peer_order(n)

    def wa_copy(i):
        return pltpu.make_async_copy((wq_hbm, wk_hbm, wv_hbm, wo_hbm)[i], wa_ref.at[i], wa_sem.at[i])

    def wf_copy(i):
        src, dst = ((w_in_hbm, w_in), (w_out_hbm, w_out))[i]
        return pltpu.make_async_copy(src, dst, wf_sem.at[i])

    def h_copy(i):
        return pltpu.make_async_copy(hbuf.at[lax.rem(i, 2)], out_hbm.at[i], h_sem.at[lax.rem(i, 2)])

    def h_back(i):
        return pltpu.make_async_copy(out_hbm.at[i], hbuf.at[lax.rem(i, 2)], h_sem.at[lax.rem(i, 2)])

    def o_copy(i):
        return pltpu.make_async_copy(obuf.at[lax.rem(i, 2)], out_hbm.at[i], o_sem.at[lax.rem(i, 2)])

    def lhs_copy(i):
        return pltpu.make_async_copy(recv_hbm.at[:, i], lhs_ref, l_sem)

    def ret_copy(i):
        return pltpu.make_async_copy(ret_hbm.at[i], retb.at[lax.rem(i, 2)], r_sem.at[lax.rem(i, 2)])

    def own_copy(i):
        return pltpu.make_async_copy(xs_ref.at[i, me], recv_hbm.at[me, i], own_sem.at[i])

    def own2_copy(i):
        return pltpu.make_async_copy(xs_ref.at[i, me], ret_hbm.at[i, me], own2_sem.at[i])

    def wait_peers(i, sem):
        block = xs_ref.at[i, pl.ds(0, n - 1)]
        pltpu.make_async_copy(block, block, sem.at[i]).wait()

    @pl.when(t == 0)
    def _():
        for i in range(4):
            wa_copy(i).start()
        barrier = pltpu.get_barrier_semaphore()
        for k in ks:
            pl.semaphore_signal(barrier, inc=1, device_id=(me ^ k,), device_id_type=MESH)
        lacc[...] = jnp.zeros_like(lacc)
        w = wg_ref[...]
        hi = w.astype(BF16)
        rest = w - hi.astype(F32)
        mid = rest.astype(BF16)
        wg3_ref[0:experts] = hi
        wg3_ref[experts:2 * experts] = mid
        wg3_ref[2 * experts:] = (rest - mid.astype(F32)).astype(BF16)

    @pl.when(t == 1)
    def _():
        pl.semaphore_wait(pltpu.get_barrier_semaphore(), n - 1)
        wf_copy(0).start()
        wf_copy(1).start()

    @pl.when((t > 0) & (t <= groups))
    def _():
        p = t - 1
        for k in ks:
            peer = me ^ k
            pltpu.make_async_remote_copy(
                src_ref=xs_ref.at[p, peer], dst_ref=recv_hbm.at[me, p],
                send_sem=send_sem.at[p], recv_sem=recv_sem.at[p],
                device_id=(peer,), device_id_type=MESH).start()
        own_copy(p).start()

    @pl.when(t == groups)
    def _():
        for k in ks:
            pltpu.make_async_remote_copy(
                src_ref=lacc, dst_ref=lbuf.at[me], send_sem=lsend_sem, recv_sem=lrecv_sem,
                device_id=(me ^ k,), device_id_type=MESH).start()
        lbuf[me] = lacc[...]
        h_copy(groups - 2).wait()
        h_copy(groups - 1).wait()
        wf_copy(0).wait()
        wf_copy(1).wait()

    @pl.when((t > groups) & (t <= 2 * groups))
    def _():
        p = t - groups - 1
        for k in ks:
            peer = me ^ k
            pltpu.make_async_remote_copy(
                src_ref=xs_ref.at[p, peer], dst_ref=ret_hbm.at[p, me],
                send_sem=send2_sem.at[p], recv_sem=recv2_sem.at[p],
                device_id=(peer,), device_id_type=MESH).start()
        own2_copy(p).start()

    @pl.when(t < groups)
    def _():
        g = t
        a = norm_rows(tok_ref[0].astype(F32), na_ref[...])
        for c in range(3):
            @pl.when(t == 0)
            def _():
                wa_copy(c).wait()
            qkv_ref[:, c * d:(c + 1) * d] = dot_nt(a, wa_ref[c]).astype(BF16)
        key_ok = mask_ref[pl.ds(g, 1), :] == 1
        low = lax.broadcasted_iota(jnp.int32, (seq, 128), 1) < 64
        factor = 0.125 * LOG2E

        def probs(q, k):
            s = jnp.where(key_ok, dot_nt(q, k), -1e30)
            e = jnp.exp2((s - jnp.max(s, axis=-1, keepdims=True)) * factor)
            return (e * (1.0 / jnp.sum(e, axis=-1, keepdims=True))).astype(BF16)

        def pair(i, carry):
            off = pl.multiple_of(i * 128, 128)
            q = qkv_ref[:, pl.ds(off, 128)]
            k = qkv_ref[:, pl.ds(pl.multiple_of(d + off, 128), 128)]
            v = qkv_ref[:, pl.ds(pl.multiple_of(2 * d + off, 128), 128)]
            zero = jnp.zeros_like(q)
            p0 = probs(jnp.where(low, q, zero), k)
            p1 = probs(jnp.where(low, zero, q), k)
            c = dot_nn(p0, jnp.where(low, v, zero))
            c += dot_nn(p1, jnp.where(low, zero, v))
            ctx_ref[:, pl.ds(off, 128)] = c.astype(BF16)
            return carry

        lax.fori_loop(0, heads // 2, pair, 0, unroll=2)

        @pl.when(t == 0)
        def _():
            wa_copy(3).wait()

        @pl.when(t >= 2)
        def _():
            h_copy(g - 2).wait()
        h = (tok_ref[0].astype(F32) + dot_nn(ctx_ref[...], wa_ref[3])).astype(BF16)
        hbuf[lax.rem(g, 2)] = h
        b = norm_rows(h.astype(F32), nm_ref[...])

        lg = dot_nt(wg3_ref[...], b)
        lg = lg[:experts] + (lg[experts:2 * experts] + lg[2 * experts:])
        ex = jnp.exp(lg - jnp.max(lg, axis=0, keepdims=True))
        p = ex / jnp.sum(ex, axis=0, keepdims=True)
        c1 = pick_ref[0, 0:1, :].astype(F32)
        c2 = pick_ref[0, 1:2, :].astype(F32)
        draw = draw_ref[pl.ds(g, 1), :]
        valid = jnp.where(key_ok, 1.0, 0.0)
        ids = lax.broadcasted_iota(jnp.int32, (experts, seq), 0).astype(F32)
        hot1 = jnp.where(ids == c1, 1.0, 0.0)
        hot2 = jnp.where(ids == c2, 1.0, 0.0)
        p1 = jnp.sum(hot1 * p, axis=0, keepdims=True)
        p2 = jnp.sum(hot2 * p, axis=0, keepdims=True)
        g1 = p1 / (p1 + p2)
        g2 = p2 / (p1 + p2)
        want2 = valid * jnp.where(draw < 2.0 * g2, 1.0, 0.0)
        take1 = hot1 * valid
        take2 = hot2 * want2
        upper = jnp.where(lax.broadcasted_iota(jnp.int32, (seq, seq), 0)
                          <= lax.broadcasted_iota(jnp.int32, (seq, seq), 1), 1.0, 0.0).astype(BF16)
        cum1 = dot_nn(take1.astype(BF16), upper)
        cum2 = dot_nn(take2.astype(BF16), upper)
        count1 = jnp.sum(take1, axis=1, keepdims=True)
        pos1 = jnp.sum((cum1 - 1.0) * take1, axis=0, keepdims=True)
        pos2 = jnp.sum((cum2 - 1.0 + jnp.minimum(count1, float(cap))) * take2, axis=0, keepdims=True)
        slot1 = jnp.where((valid > 0.5) & (pos1 < float(cap)), c1 * float(cap) + pos1, -1.0)
        slot2 = jnp.where((want2 > 0.5) & (pos2 < float(cap)), c2 * float(cap) + pos2, -1.0)
        half = experts * cap // 2
        for part in range(2):
            slots = lax.broadcasted_iota(jnp.int32, (half, seq), 0).astype(F32) + float(part * half)
            pick = jnp.where((slots == slot1) | (slots == slot2), 1.0, 0.0).astype(BF16)
            xs_ref[g, part * (n // 2):(part + 1) * (n // 2)] = dot_nn(pick, b).astype(BF16).reshape(n // 2, rows, d)
        density = jnp.sum(p * valid, axis=1, keepdims=True) * (1.0 / seq)
        lacc[...] += jnp.sum(count1 * (1.0 / seq) * density, axis=0, keepdims=True)
        aux_ref[g] = jnp.concatenate([slot1, slot2, g1, g2, g1, g1, g1, g1], axis=0)
        h_copy(g).start()

    @pl.when((t >= groups) & (t < 2 * groups))
    def _():
        r = t - groups
        wait_peers(r, recv_sem)
        own_copy(r).wait()
        lhs_copy(r).start()
        wait_peers(r, send_sem)
        lhs_copy(r).wait()
        for e in range(e_loc):
            lhs = lhs_ref[:, e * cap:(e + 1) * cap, :].reshape(n * cap, d)
            for c in range(2):
                cols = slice(c * (ff // 2), (c + 1) * (ff // 2))
                mid_ref[:, cols] = jnp.maximum(dot_nn(lhs, w_in[e, :, cols]), 0.0).astype(BF16)
            for c in range(2):
                cols = slice(c * (d // 2), (c + 1) * (d // 2))
                down = dot_nn(mid_ref[...], w_out[e, :, cols]).astype(BF16)
                xs_ref[r, :, e * cap:(e + 1) * cap, cols] = down.reshape(n, cap, d // 2)

    @pl.when((t >= 2 * groups) & (t < 3 * groups))
    def _():
        g = t - 2 * groups
        wait_peers(g, recv2_sem)
        own2_copy(g).wait()
        ret_copy(g).start()
        h_back(g).start()

    @pl.when(t > 2 * groups)
    def _():
        g = t - 2 * groups - 1
        slot1 = aux_ref[g, 0:1, :]
        slot2 = aux_ref[g, 1:2, :]
        g1 = aux_ref[g, 2:3, :]
        g2 = aux_ref[g, 3:4, :]
        ids = lax.broadcasted_iota(jnp.int32, (n * rows, seq), 0).astype(F32)
        comb = (jnp.where(ids == slot1, g1, 0.0) + jnp.where(ids == slot2, g2, 0.0)).astype(BF16)

        @pl.when(g >= 2)
        def _():
            o_copy(g - 2).wait()
        ret_copy(g).wait()
        h_back(g).wait()
        b = lax.rem(g, 2)
        moe = dot_tn(comb, retb[b].reshape(n * rows, d))
        obuf[b] = (hbuf[b].astype(F32) + moe).astype(BF16)
        o_copy(g).start()

    @pl.when(t == 3 * groups)
    def _():
        o_copy(groups - 2).wait()
        o_copy(groups - 1).wait()
        for i in range(groups):
            wait_peers(i, send2_sem)
        block = lbuf.at[pl.ds(0, n - 1)]
        pltpu.make_async_copy(block, block, lsend_sem).wait()
        pltpu.make_async_copy(block, block, lrecv_sem).wait()
        total = jnp.sum(lbuf[...], axis=0)
        loss_ref[...] = total[0:1, 0:1] * float(experts) / float(groups * n)


def solution(mesh):
    n = mesh.shape["ep"]

    def local_step(tokens, pad_mask, second_draw, choices, norm_attn, w_query, w_key, w_value, w_attn_out, norm_moe, w_gate, w_in, w_out):
        groups, seq, d = tokens.shape
        heads = w_query.shape[1]
        experts = w_gate.shape[1]
        e_loc, _, ff = w_in.shape
        cap = (2 * seq + experts - 1) // experts
        rows = e_loc * cap
        turned = [jnp.transpose(w, (1, 2, 0)).reshape(d, d) for w in (w_query, w_key, w_value)]
        wo = w_attn_out.reshape(d, d)
        last = groups - 1
        hbm = pl.BlockSpec(memory_space=pl.ANY)

        def whole(shape):
            return pl.BlockSpec(shape, lambda t: (0,) * len(shape), pipeline_mode=pl.Buffered(1))

        dma = pltpu.SemaphoreType.DMA
        out, loss, _, _ = pl.pallas_call(
            functools.partial(layer_kernel, n, heads, cap, groups),
            grid=(3 * groups + 1,),
            out_shape=(jax.ShapeDtypeStruct((groups, seq, d), BF16),
                       jax.ShapeDtypeStruct((1, 1), F32),
                       jax.ShapeDtypeStruct((n, groups, rows, d), BF16),
                       jax.ShapeDtypeStruct((groups, n, rows, d), BF16)),
            in_specs=[whole((groups, seq)), whole((groups, seq)),
                      pl.BlockSpec((1, 2, seq), lambda t: (jnp.minimum(t, last), 0, 0)),
                      pl.BlockSpec((1, seq, d), lambda t: (jnp.minimum(t, last), 0, 0)),
                      whole((1, d)), whole((1, d)), whole((experts, d))] + [hbm] * 6,
            out_specs=(hbm, pl.BlockSpec((1, 1), lambda t: (0, 0)), hbm, hbm),
            scratch_shapes=[pltpu.VMEM((4, d, d), BF16), pltpu.VMEM((3 * experts, d), BF16),
                            pltpu.VMEM((seq, 3 * d), BF16), pltpu.VMEM((seq, d), BF16),
                            pltpu.VMEM((2, seq, d), BF16), pltpu.VMEM((2, seq, d), BF16),
                            pltpu.VMEM((groups, 8, seq), F32), pltpu.VMEM((8, 128), F32),
                            pltpu.VMEM((n, 8, 128), F32), pltpu.VMEM((groups, n, rows, d), BF16),
                            pltpu.VMEM((e_loc, d, ff), BF16), pltpu.VMEM((e_loc, ff, d), BF16),
                            pltpu.VMEM((n * cap, ff), BF16), pltpu.VMEM((n, rows, d), BF16),
                            pltpu.VMEM((2, n, rows, d), BF16),
                            dma((4,)), dma((2,)), dma((2,)), dma((2,)), dma, dma((2,)),
                            dma((groups,)), dma((groups,)), dma((groups,)), dma((groups,)),
                            dma((groups,)), dma((groups,)), dma, dma],
            compiler_params=pltpu.CompilerParams(collective_id=0, has_side_effects=True,
                                                 vmem_limit_bytes=67043328),
        )(pad_mask, second_draw, jnp.transpose(choices, (0, 2, 1)), tokens,
          norm_attn.reshape(1, d), norm_moe.reshape(1, d), w_gate.T, *turned, wo, w_in, w_out)
        return out, loss[0, 0]

    by_group = P("ep")
    replicated = P()
    in_specs = (by_group, by_group, by_group, by_group, replicated, replicated, replicated, replicated, replicated, replicated, replicated, by_group, by_group)
    return jax.shard_map(local_step, mesh=mesh, in_specs=in_specs, out_specs=(by_group, replicated), check_vma=False)
```

```python
import functools
import jax
import jax.numpy as jnp
from jax import lax
from jax.experimental import pallas as pl
from jax.experimental.pallas import tpu as pltpu
from jax.sharding import PartitionSpec as P

NORM_EPS = 1e-6
MESH = pl.DeviceIdType.MESH
F32 = jnp.float32
BF16 = jnp.bfloat16
LOG2E = 1.4426950408889634
O_ROUNDS = 5
INNER = 3


def norm_rows(x, scale):
    inv = lax.rsqrt(jnp.mean(x * x, axis=-1, keepdims=True) + NORM_EPS)
    return (x * inv * scale).astype(BF16)


def dot_nn(a, b):
    return jnp.dot(a, b, preferred_element_type=F32)


def dot_nt(a, b):
    return lax.dot_general(a, b, (((1,), (1,)), ((), ())), preferred_element_type=F32)


def dot_tn(a, b):
    return lax.dot_general(a, b, (((0,), (0,)), ((), ())), preferred_element_type=F32)


def peer_order(n):
    full = [2, 4, 8, 3, 5, 9, 6, 12, 10, 7, 13, 11, 14, 15, 1]
    return full if n == 16 else list(range(1, n))


def attend_heads(qkv_ref, ctx_ref, key_ok, heads):
    seq, d = ctx_ref.shape
    low = lax.broadcasted_iota(jnp.int32, (seq, 128), 1) < 64
    factor = 0.125 * LOG2E

    def probs(q, k):
        s = jnp.where(key_ok, dot_nt(q, k), -1e30)
        e = jnp.exp2((s - jnp.max(s, axis=-1, keepdims=True)) * factor)
        return (e * (1.0 / jnp.sum(e, axis=-1, keepdims=True))).astype(BF16)

    def pair(i, carry):
        off = pl.multiple_of(i * 128, 128)
        q = qkv_ref[:, pl.ds(off, 128)]
        k = qkv_ref[:, pl.ds(pl.multiple_of(d + off, 128), 128)]
        v = qkv_ref[:, pl.ds(pl.multiple_of(2 * d + off, 128), 128)]
        zero = jnp.zeros_like(q)
        p0 = probs(jnp.where(low, q, zero), k)
        p1 = probs(jnp.where(low, zero, q), k)
        c = dot_nn(p0, jnp.where(low, v, zero))
        c += dot_nn(p1, jnp.where(low, zero, v))
        ctx_ref[:, pl.ds(off, 128)] = c.astype(BF16)
        return carry

    lax.fori_loop(0, heads // 2, pair, 0, unroll=4)


def gate(wg3_ref, b, pick_ref, draw, key_ok, cap):
    experts, seq = wg3_ref.shape[0] // 3, b.shape[0]
    lg = dot_nt(wg3_ref[...], b)
    lg = lg[:experts] + (lg[experts:2 * experts] + lg[2 * experts:])
    ex = jnp.exp(lg - jnp.max(lg, axis=0, keepdims=True))
    p = ex / jnp.sum(ex, axis=0, keepdims=True)
    c1 = pick_ref[0, 0:1, :].astype(F32)
    c2 = pick_ref[0, 1:2, :].astype(F32)
    valid = jnp.where(key_ok, 1.0, 0.0)
    ids = lax.broadcasted_iota(jnp.int32, (experts, seq), 0).astype(F32)
    hot1 = jnp.where(ids == c1, 1.0, 0.0)
    hot2 = jnp.where(ids == c2, 1.0, 0.0)
    p1 = jnp.sum(hot1 * p, axis=0, keepdims=True)
    p2 = jnp.sum(hot2 * p, axis=0, keepdims=True)
    g1 = p1 / (p1 + p2)
    g2 = p2 / (p1 + p2)
    want2 = valid * jnp.where(draw < 2.0 * g2, 1.0, 0.0)
    take1 = hot1 * valid
    take2 = hot2 * want2
    upper = jnp.where(lax.broadcasted_iota(jnp.int32, (seq, seq), 0)
                      <= lax.broadcasted_iota(jnp.int32, (seq, seq), 1), 1.0, 0.0).astype(BF16)
    cum1 = dot_nn(take1.astype(BF16), upper)
    cum2 = dot_nn(take2.astype(BF16), upper)
    count1 = jnp.sum(take1, axis=1, keepdims=True)
    pos1 = jnp.sum((cum1 - 1.0) * take1, axis=0, keepdims=True)
    pos2 = jnp.sum((cum2 - 1.0 + jnp.minimum(count1, float(cap))) * take2, axis=0, keepdims=True)
    return p, c1, c2, valid, hot1, hot2, g1, g2, want2, take2, count1, pos1, pos2


def layer_kernel(n, heads, cap, groups, mask_ref, draw_ref, pick_ref, tok_ref, na_ref, nm_ref, wg_ref,
                 wq_hbm, wk_hbm, wv_hbm, wo_hbm, w_in_hbm, w_out_hbm,
                 out_hbm, loss_ref, recv_hbm, ret_hbm,
                 wa_ref, wg3_ref, qkv_ref, ctx_ref, hbuf, obuf, aux_ref, lacc, lbuf, xs_ref,
                 w_in, w_out, mid_ref, lhs_ref, retb,
                 wa_sem, wf_sem, h_sem, o_sem, l_sem, r_sem, own_sem, own2_sem,
                 send_sem, recv_sem, send2_sem, recv2_sem, lsend_sem, lrecv_sem):
    me = lax.axis_index("ep")
    t = pl.program_id(0)
    seq, d = tok_ref.shape[1], tok_ref.shape[2]
    experts = wg_ref.shape[0]
    e_loc, _, ff = w_in.shape
    rows = e_loc * cap
    ks = peer_order(n)

    def wa_copy(i):
        return pltpu.make_async_copy((wq_hbm, wk_hbm, wv_hbm, wo_hbm)[i], wa_ref.at[i], wa_sem.at[i])

    def wf_copy(i):
        src, dst = ((w_in_hbm, w_in), (w_out_hbm, w_out))[i]
        return pltpu.make_async_copy(src, dst, wf_sem.at[i])

    def h_copy(i):
        return pltpu.make_async_copy(hbuf.at[lax.rem(i, 2)], out_hbm.at[i], h_sem.at[lax.rem(i, 2)])

    def h_back(i):
        return pltpu.make_async_copy(out_hbm.at[i], hbuf.at[lax.rem(i, 2)], h_sem.at[lax.rem(i, 2)])

    def o_copy(i):
        return pltpu.make_async_copy(obuf.at[lax.rem(i, 2)], out_hbm.at[i], o_sem.at[lax.rem(i, 2)])

    def lhs_copy(i):
        return pltpu.make_async_copy(recv_hbm.at[:, i], lhs_ref, l_sem)

    def ret_copy(i):
        return pltpu.make_async_copy(ret_hbm.at[i], retb.at[lax.rem(i, 2)], r_sem.at[lax.rem(i, 2)])

    def own_copy(i):
        return pltpu.make_async_copy(xs_ref.at[i, me], recv_hbm.at[me, i], own_sem.at[i])

    def own2_copy(i):
        return pltpu.make_async_copy(xs_ref.at[i, me], ret_hbm.at[i, me], own2_sem.at[i])

    def wait_peers(i, sem):
        block = xs_ref.at[i, pl.ds(0, n - 1)]
        pltpu.make_async_copy(block, block, sem.at[i]).wait()

    @pl.when(t == 0)
    def _():
        for i in range(4):
            wa_copy(i).start()
        barrier = pltpu.get_barrier_semaphore()
        for k in ks:
            pl.semaphore_signal(barrier, inc=1, device_id=(me ^ k,), device_id_type=MESH)
        lacc[...] = jnp.zeros_like(lacc)
        w = wg_ref[...]
        hi = w.astype(BF16)
        rest = w - hi.astype(F32)
        mid = rest.astype(BF16)
        wg3_ref[0:experts] = hi
        wg3_ref[experts:2 * experts] = mid
        wg3_ref[2 * experts:] = (rest - mid.astype(F32)).astype(BF16)

    @pl.when(t == 1)
    def _():
        pl.semaphore_wait(pltpu.get_barrier_semaphore(), n - 1)
        wf_copy(0).start()
        wf_copy(1).start()

    @pl.when((t > 0) & (t <= groups))
    def _():
        p = t - 1
        for k in ks:
            peer = me ^ k
            pltpu.make_async_remote_copy(
                src_ref=xs_ref.at[p, peer], dst_ref=recv_hbm.at[me, p],
                send_sem=send_sem.at[p], recv_sem=recv_sem.at[p],
                device_id=(peer,), device_id_type=MESH).start()
        own_copy(p).start()

    @pl.when(t == groups)
    def _():
        for k in ks:
            pltpu.make_async_remote_copy(
                src_ref=lacc, dst_ref=lbuf.at[me], send_sem=lsend_sem, recv_sem=lrecv_sem,
                device_id=(me ^ k,), device_id_type=MESH).start()
        lbuf[me] = lacc[...]
        h_copy(groups - 2).wait()
        h_copy(groups - 1).wait()
        wf_copy(0).wait()
        wf_copy(1).wait()

    @pl.when((t > groups) & (t <= 2 * groups))
    def _():
        p = t - groups - 1
        for k in ks:
            peer = me ^ k
            pltpu.make_async_remote_copy(
                src_ref=xs_ref.at[p, peer], dst_ref=ret_hbm.at[p, me],
                send_sem=send2_sem.at[p], recv_sem=recv2_sem.at[p],
                device_id=(peer,), device_id_type=MESH).start()
        own2_copy(p).start()

    @pl.when(t < groups)
    def _():
        g = t
        a = norm_rows(tok_ref[0].astype(F32), na_ref[...])
        for c in range(3):
            @pl.when(t == 0)
            def _():
                wa_copy(c).wait()
            qkv_ref[:, c * d:(c + 1) * d] = dot_nt(a, wa_ref[c]).astype(BF16)
        key_ok = mask_ref[pl.ds(g, 1), :] == 1
        attend_heads(qkv_ref, ctx_ref, key_ok, heads)

        @pl.when(t == 0)
        def _():
            wa_copy(3).wait()

        @pl.when(t >= 2)
        def _():
            h_copy(g - 2).wait()
        h = (tok_ref[0].astype(F32) + dot_nn(ctx_ref[...], wa_ref[3])).astype(BF16)
        hbuf[lax.rem(g, 2)] = h
        b = norm_rows(h.astype(F32), nm_ref[...])

        p, c1, c2, valid, hot1, hot2, g1, g2, want2, take2, count1, pos1, pos2 = gate(
            wg3_ref, b, pick_ref, draw_ref[pl.ds(g, 1), :], key_ok, cap)
        slot1 = jnp.where((valid > 0.5) & (pos1 < float(cap)), c1 * float(cap) + pos1, -1.0)
        slot2 = jnp.where((want2 > 0.5) & (pos2 < float(cap)), c2 * float(cap) + pos2, -1.0)
        half = experts * cap // 2
        for part in range(2):
            slots = lax.broadcasted_iota(jnp.int32, (half, seq), 0).astype(F32) + float(part * half)
            pick = jnp.where((slots == slot1) | (slots == slot2), 1.0, 0.0).astype(BF16)
            xs_ref[g, part * (n // 2):(part + 1) * (n // 2)] = dot_nn(pick, b).astype(BF16).reshape(n // 2, rows, d)
        density = jnp.sum(p * valid, axis=1, keepdims=True) * (1.0 / seq)
        lacc[...] += jnp.sum(count1 * (1.0 / seq) * density, axis=0, keepdims=True)
        aux_ref[g] = jnp.concatenate([slot1, slot2, g1, g2, g1, g1, g1, g1], axis=0)
        h_copy(g).start()

    @pl.when((t >= groups) & (t < 2 * groups))
    def _():
        r = t - groups
        wait_peers(r, recv_sem)
        own_copy(r).wait()
        lhs_copy(r).start()
        wait_peers(r, send_sem)
        lhs_copy(r).wait()
        for e in range(e_loc):
            lhs = lhs_ref[:, e * cap:(e + 1) * cap, :].reshape(n * cap, d)
            for c in range(2):
                cols = slice(c * (ff // 2), (c + 1) * (ff // 2))
                mid_ref[:, cols] = jnp.maximum(dot_nn(lhs, w_in[e, :, cols]), 0.0).astype(BF16)
            for c in range(2):
                cols = slice(c * (d // 2), (c + 1) * (d // 2))
                down = dot_nn(mid_ref[...], w_out[e, :, cols]).astype(BF16)
                xs_ref[r, :, e * cap:(e + 1) * cap, cols] = down.reshape(n, cap, d // 2)

    @pl.when((t >= 2 * groups) & (t < 3 * groups))
    def _():
        g = t - 2 * groups
        wait_peers(g, recv2_sem)
        own2_copy(g).wait()
        ret_copy(g).start()
        h_back(g).start()

    @pl.when(t > 2 * groups)
    def _():
        g = t - 2 * groups - 1
        slot1 = aux_ref[g, 0:1, :]
        slot2 = aux_ref[g, 1:2, :]
        g1 = aux_ref[g, 2:3, :]
        g2 = aux_ref[g, 3:4, :]
        ids = lax.broadcasted_iota(jnp.int32, (n * rows, seq), 0).astype(F32)
        comb = (jnp.where(ids == slot1, g1, 0.0) + jnp.where(ids == slot2, g2, 0.0)).astype(BF16)

        @pl.when(g >= 2)
        def _():
            o_copy(g - 2).wait()
        ret_copy(g).wait()
        h_back(g).wait()
        b = lax.rem(g, 2)
        moe = dot_tn(comb, retb[b].reshape(n * rows, d))
        obuf[b] = (hbuf[b].astype(F32) + moe).astype(BF16)
        o_copy(g).start()

    @pl.when(t == 3 * groups)
    def _():
        o_copy(groups - 2).wait()
        o_copy(groups - 1).wait()
        for i in range(groups):
            wait_peers(i, send2_sem)
        block = lbuf.at[pl.ds(0, n - 1)]
        pltpu.make_async_copy(block, block, lsend_sem).wait()
        pltpu.make_async_copy(block, block, lrecv_sem).wait()
        total = jnp.sum(lbuf[...], axis=0)
        loss_ref[...] = total[0:1, 0:1] * float(experts) / float(groups * n)


def packed_kernel(n, heads, cap, groups, s_rounds, o_rounds, inner, mask_ref, draw_ref, pick_ref, tok_ref, na_ref, nm_ref, wg_ref,
                  wq_hbm, wk_hbm, wv_hbm, wo_hbm, w_in_hbm, w_out_hbm,
                  out_hbm, loss_ref, flag_ref, recv_hbm, ret_hbm,
                  wa_ref, wg3_ref, qkv_ref, ctx_ref, hbuf, acc_ref, aux_ref, base_ref, lacc, lbuf, xs_ref, ball_ref,
                  w_in, w_out,
                  wa_sem, wf_sem, h_sem, o_sem, l_sem, r_sem, own_sem, own2_sem,
                  send_sem, recv_sem, send2_sem, recv2_sem, lsend_sem, lrecv_sem):
    me = lax.axis_index("ep")
    t = pl.program_id(0)
    seq, d = tok_ref.shape[1], tok_ref.shape[2]
    experts = wg_ref.shape[0]
    e_loc, _, ff = w_in.shape
    rows = e_loc * cap
    full = n * rows
    low_cap = cap // 2
    rounds = s_rounds + o_rounds
    t_over = 3 * s_rounds
    t_ffn = t_over + o_rounds
    t_comb = t_ffn + rounds - inner
    couple, part_of = t // 3, lax.rem(t, 3)
    in_front = t < t_over
    over_max = float(o_rounds * cap)
    ks = peer_order(n)

    def my_rows(i):
        return pl.ds(pl.multiple_of(i * rows, rows), rows)

    def wa_copy(i):
        return pltpu.make_async_copy((wq_hbm, wk_hbm, wv_hbm, wo_hbm)[i], wa_ref.at[i], wa_sem.at[i])

    def wf_copy(i):
        src, dst = ((w_in_hbm, w_in), (w_out_hbm, w_out))[i]
        return pltpu.make_async_copy(src, dst, wf_sem.at[i])

    def h_copy(i):
        b = lax.rem(i, 2)
        return pltpu.make_async_copy(hbuf.at[b, 0], out_hbm.at[i], h_sem.at[b])

    def h_back(i):
        b = lax.rem(i, 2)
        return pltpu.make_async_copy(out_hbm.at[pl.ds(2 * i, 2)], hbuf.at[b], h_sem.at[b])

    def o_copy(i):
        b = lax.rem(i, 2)
        return pltpu.make_async_copy(hbuf.at[b], out_hbm.at[pl.ds(2 * i, 2)], o_sem.at[b])

    def lhs_copy(i):
        return [pltpu.make_async_copy(recv_hbm.at[i, pl.ds(b * seq, seq)], hbuf.at[b, 1], l_sem.at[b]) for b in range(2)]

    def ret_copy(i):
        return pltpu.make_async_copy(ret_hbm.at[i], wa_ref.at[1, pl.ds(0, full)], r_sem)

    def over_copy(i):
        return pltpu.make_async_copy(ret_hbm.at[s_rounds + i], ball_ref.at[pl.ds(i * full, full)], wa_sem.at[0])

    def own_copy(i):
        return pltpu.make_async_copy(xs_ref.at[i, me], recv_hbm.at[i, my_rows(me)], own_sem.at[i])

    def own2_copy(i):
        return pltpu.make_async_copy(xs_ref.at[i, me], ret_hbm.at[i, my_rows(me)], own2_sem.at[i])

    def wait_peers(i, sem):
        block = xs_ref.at[i, pl.ds(0, n - 1)]
        pltpu.make_async_copy(block, block, sem.at[i]).wait()

    def round_of(i):
        return jnp.where(i < 1, inner, jnp.where(i <= o_rounds, i - 1 + s_rounds, i - o_rounds + inner))

    def inner_of(c):
        return (c >= 2) & (c < 2 + inner)

    def row_ids(count, start):
        return (lax.broadcasted_iota(jnp.int32, (count, seq), 0) + start).astype(F32)

    def pick_rows(ids, g, first):
        one = aux_ref[g, first:first + 1, :]
        two = aux_ref[g, first + 1:first + 2, :]
        return jnp.where((ids == one) | (ids == two), 1.0, 0.0).astype(BF16)

    def gate_rows(ids, g, first):
        one = aux_ref[g, first:first + 1, :]
        two = aux_ref[g, first + 1:first + 2, :]
        return (jnp.where(ids == one, aux_ref[g, 4:5, :], 0.0)
                + jnp.where(ids == two, aux_ref[g, 5:6, :], 0.0)).astype(BF16)

    @pl.when(t == 0)
    def _():
        for i in range(4):
            wa_copy(i).start()
        barrier = pltpu.get_barrier_semaphore()
        for k in ks:
            pl.semaphore_signal(barrier, inc=1, device_id=(me ^ k,), device_id_type=MESH)
        lacc[...] = jnp.zeros_like(lacc)
        base_ref[...] = jnp.zeros_like(base_ref)
        w = wg_ref[...]
        hi = w.astype(BF16)
        rest = w - hi.astype(F32)
        mid = rest.astype(BF16)
        wg3_ref[0:experts] = hi
        wg3_ref[experts:2 * experts] = mid
        wg3_ref[2 * experts:] = (rest - mid.astype(F32)).astype(BF16)

    @pl.when(t == 1)
    def _():
        pl.semaphore_wait(pltpu.get_barrier_semaphore(), n - 1)
        wf_copy(0).start()
        wf_copy(1).start()

    @pl.when((in_front & (part_of == 2)) | ((t > t_over) & (t <= t_ffn)))
    def _():
        p = jnp.where(in_front, couple, t - t_over - 1 + s_rounds)
        for k in ks:
            peer = me ^ k
            pltpu.make_async_remote_copy(
                src_ref=xs_ref.at[p, peer], dst_ref=recv_hbm.at[p, my_rows(me)],
                send_sem=send_sem.at[p], recv_sem=recv_sem.at[p],
                device_id=(peer,), device_id_type=MESH).start()
        own_copy(p).start()

    @pl.when(t == t_over)
    def _():
        over = jnp.sum(jnp.where(base_ref[:, 0:1] > over_max, 1.0, 0.0), axis=0, keepdims=True)
        top = lax.broadcasted_iota(jnp.int32, lacc.shape, 0) < 4
        lacc[...] = jnp.where(top, lacc[...], over)
        h_copy(groups - 2).wait()
        h_copy(groups - 1).wait()

    @pl.when(t == 8)
    def _():
        wf_copy(0).wait()
        wf_copy(1).wait()

    @pl.when(t == t_over + 1)
    def _():
        for k in ks:
            pltpu.make_async_remote_copy(
                src_ref=lacc, dst_ref=lbuf.at[me], send_sem=lsend_sem, recv_sem=lrecv_sem,
                device_id=(me ^ k,), device_id_type=MESH).start()
        lbuf[me] = lacc[...]

    @pl.when((in_front & (part_of == 0) & inner_of(couple - 1)) | ((t > t_ffn) & (t <= t_comb)))
    def _():
        p = jnp.where(in_front, couple - 3, round_of(t - t_ffn - 1))
        for k in ks:
            peer = me ^ k
            pltpu.make_async_remote_copy(
                src_ref=xs_ref.at[p, peer], dst_ref=ret_hbm.at[p, my_rows(me)],
                send_sem=send2_sem.at[p], recv_sem=recv2_sem.at[p],
                device_id=(peer,), device_id_type=MESH).start()
        own2_copy(p).start()

    @pl.when(in_front & (part_of < 2))
    def _():
        g = 2 * couple + part_of
        a = norm_rows(tok_ref[0].astype(F32), na_ref[...])
        for c in range(3):
            @pl.when(t == 0)
            def _():
                wa_copy(c).wait()
            qkv_ref[:, c * d:(c + 1) * d] = dot_nt(a, wa_ref[c]).astype(BF16)
        key_ok = mask_ref[pl.ds(g, 1), :] == 1
        attend_heads(qkv_ref, ctx_ref, key_ok, heads)

        @pl.when(t == 0)
        def _():
            wa_copy(3).wait()

        @pl.when(g >= 2)
        def _():
            h_copy(g - 2).wait()
        h = (tok_ref[0].astype(F32) + dot_nn(ctx_ref[...], wa_ref[3])).astype(BF16)
        hbuf[lax.rem(g, 2), 0] = h
        b = norm_rows(h.astype(F32), nm_ref[...])
        ball_ref[pl.ds(pl.multiple_of(g * seq, seq), seq), :] = b

        p, c1, c2, valid, hot1, hot2, g1, g2, want2, take2, count1, pos1, pos2 = gate(
            wg3_ref, b, pick_ref, draw_ref[pl.ds(g, 1), :], key_ok, cap)
        keep1 = (valid > 0.5) & (pos1 < float(cap))
        keep2 = (want2 > 0.5) & (pos2 < float(cap))
        low = float(low_cap)
        base = base_ref[:, 0:1]
        parity = (lax.rem(g, 2) * low_cap).astype(F32)

        def place(keep, hot, chosen, pos):
            fixed = jnp.where(keep & (pos < low), chosen * float(cap) + parity + pos, -1.0)
            q = jnp.sum(hot * base, axis=0, keepdims=True) + pos - low
            block = jnp.floor(q * (1.0 / cap))
            packed = block * float(full) + chosen * float(cap) + (q - block * float(cap))
            return fixed, jnp.where(keep & (pos >= low) & (q < over_max), packed, -1.0)

        s1, o1 = place(keep1, hot1, c1, pos1)
        s2, o2 = place(keep2, hot2, c2, pos2)
        kept = jnp.minimum(count1 + jnp.sum(take2, axis=1, keepdims=True), float(cap))
        base_ref[...] += jnp.maximum(kept - low, 0.0)
        aux_ref[g] = jnp.concatenate([s1, s2, o1, o2, g1, g2, g1, g1], axis=0)
        density = jnp.sum(p * valid, axis=1, keepdims=True) * (1.0 / seq)
        lacc[...] += jnp.sum(count1 * (1.0 / seq) * density, axis=0, keepdims=True)
        h_copy(g).start()

        @pl.when(part_of == 1)
        def _():
            both = ball_ref[pl.ds(pl.multiple_of((g - 1) * seq, seq), 2 * seq), :]
            for part in range(2):
                ids = row_ids(full // 2, part * (full // 2))
                pick = jnp.concatenate([pick_rows(ids, g - 1, 0), pick_rows(ids, g, 0)], axis=1)
                xs_ref[g // 2, part * (n // 2):(part + 1) * (n // 2)] = dot_nn(pick, both).astype(BF16).reshape(n // 2, rows, d)

    @pl.when((t >= t_over) & (t < t_ffn))
    def _():
        j = t - t_over
        quad = 4
        for part in range(2):
            ids = row_ids(full // 2, j * full + part * (full // 2))
            acc_ref[...] = jnp.zeros_like(acc_ref)

            def chunk(c, carry):
                picks = [pick_rows(ids, c * quad + u, 2) for u in range(quad)]
                span = ball_ref[pl.ds(pl.multiple_of(c * quad * seq, quad * seq), quad * seq), :]
                acc_ref[0] += dot_nn(jnp.concatenate(picks, axis=1), span)
                return carry

            lax.fori_loop(0, groups // quad, chunk, 0)
            xs_ref[s_rounds + j, part * (n // 2):(part + 1) * (n // 2)] = acc_ref[0].astype(BF16).reshape(n // 2, rows, d)

    @pl.when((in_front & (part_of == 2) & inner_of(couple)) | ((t >= t_ffn) & (t < t_comb)))
    def _():
        r = jnp.where(in_front, couple - 2, round_of(t - t_ffn))
        wait_peers(r, recv_sem)
        own_copy(r).wait()
        for copy in lhs_copy(r):
            copy.start()
        wait_peers(r, send_sem)
        for copy in lhs_copy(r):
            copy.wait()
        for e in range(e_loc):
            lhs = jnp.concatenate([hbuf[b, 1].reshape(n // 2, rows, d)[:, e * cap:(e + 1) * cap, :].reshape(seq // 2, d)
                                   for b in range(2)], axis=0)
            for c in range(2):
                cols = slice(c * (ff // 2), (c + 1) * (ff // 2))
                qkv_ref[:, cols] = jnp.maximum(dot_nn(lhs, w_in[e, :, cols]), 0.0).astype(BF16)
            for c in range(2):
                cols = slice(c * (d // 2), (c + 1) * (d // 2))
                down = dot_nn(qkv_ref[:, 0:ff], w_out[e, :, cols]).astype(BF16)
                xs_ref[r, :, e * cap:(e + 1) * cap, cols] = down.reshape(n, cap, d // 2)

    @pl.when(t == t_comb)
    def _():
        for i in range(o_rounds):
            wait_peers(s_rounds + i, recv2_sem)
            own2_copy(s_rounds + i).wait()
            over_copy(i).start()
            over_copy(i).wait()

    @pl.when(t >= t_comb)
    def _():
        i = t - t_comb

        @pl.when(i >= 2)
        def _():
            o_copy(i - 2).wait()
        h_back(i).start()
        acc_ref[...] = jnp.zeros_like(acc_ref)

        def both(start, first):
            ids = row_ids(full, start)
            return jnp.concatenate([gate_rows(ids, 2 * i + u, first) for u in range(2)], axis=1)

        def chunk(c, carry):
            moe = dot_tn(both(c * full, 2), ball_ref[pl.ds(pl.multiple_of(c * full, full), full), :])
            acc_ref[...] += moe.reshape(2, seq, d)
            return carry

        lax.fori_loop(0, o_rounds, chunk, 0)
        comb = both(0, 0)
        wait_peers(i, recv2_sem)
        own2_copy(i).wait()
        ret_copy(i).start()
        h_back(i).wait()
        ret_copy(i).wait()
        b = lax.rem(i, 2)
        moe = acc_ref[...] + dot_tn(comb, wa_ref[1, 0:full]).reshape(2, seq, d)
        hbuf[b] = (hbuf[b].astype(F32) + moe).astype(BF16)
        o_copy(i).start()

    @pl.when(t == t_comb + s_rounds - 1)
    def _():
        o_copy(s_rounds - 2).wait()
        o_copy(s_rounds - 1).wait()
        for i in range(rounds):
            wait_peers(i, send2_sem)
        block = lbuf.at[pl.ds(0, n - 1)]
        pltpu.make_async_copy(block, block, lsend_sem).wait()
        pltpu.make_async_copy(block, block, lrecv_sem).wait()
        total = jnp.sum(lbuf[...], axis=0)
        loss_ref[...] = total[0:1, 0:1] * float(experts) / float(groups * n)
        flag_ref[...] = total[4:5, 0:1]


def solution(mesh):
    n = mesh.shape["ep"]

    def local_step(tokens, pad_mask, second_draw, choices, norm_attn, w_query, w_key, w_value, w_attn_out, norm_moe, w_gate, w_in, w_out):
        groups, seq, d = tokens.shape
        heads = w_query.shape[1]
        experts = w_gate.shape[1]
        e_loc, _, ff = w_in.shape
        cap = (2 * seq + experts - 1) // experts
        rows = e_loc * cap
        turned = [jnp.transpose(w, (1, 2, 0)).reshape(d, d) for w in (w_query, w_key, w_value)]
        wo = w_attn_out.reshape(d, d)
        last = groups - 1
        hbm = pl.BlockSpec(memory_space=pl.ANY)

        def whole(shape):
            return pl.BlockSpec(shape, lambda t: (0,) * len(shape), pipeline_mode=pl.Buffered(1))

        dma = pltpu.SemaphoreType.DMA
        operands = (pad_mask, second_draw, jnp.transpose(choices, (0, 2, 1)), tokens,
                    norm_attn.reshape(1, d), norm_moe.reshape(1, d), w_gate.T, *turned, wo, w_in, w_out)

        def group_blocks(group_of):
            return [whole((groups, seq)), whole((groups, seq)),
                    pl.BlockSpec((1, 2, seq), lambda t: (group_of(t), 0, 0)),
                    pl.BlockSpec((1, seq, d), lambda t: (group_of(t), 0, 0)),
                    whole((1, d)), whole((1, d)), whole((experts, d))] + [hbm] * 6

        def full_layer():
            return pl.pallas_call(
                functools.partial(layer_kernel, n, heads, cap, groups),
                grid=(3 * groups + 1,),
                out_shape=(jax.ShapeDtypeStruct((groups, seq, d), BF16),
                           jax.ShapeDtypeStruct((1, 1), F32),
                           jax.ShapeDtypeStruct((n, groups, rows, d), BF16),
                           jax.ShapeDtypeStruct((groups, n, rows, d), BF16)),
                in_specs=group_blocks(lambda t: jnp.minimum(t, last)),
                out_specs=(hbm, pl.BlockSpec((1, 1), lambda t: (0, 0)), hbm, hbm),
                scratch_shapes=[pltpu.VMEM((4, d, d), BF16), pltpu.VMEM((3 * experts, d), BF16),
                                pltpu.VMEM((seq, 3 * d), BF16), pltpu.VMEM((seq, d), BF16),
                                pltpu.VMEM((2, seq, d), BF16), pltpu.VMEM((2, seq, d), BF16),
                                pltpu.VMEM((groups, 8, seq), F32), pltpu.VMEM((8, 128), F32),
                                pltpu.VMEM((n, 8, 128), F32), pltpu.VMEM((groups, n, rows, d), BF16),
                                pltpu.VMEM((e_loc, d, ff), BF16), pltpu.VMEM((e_loc, ff, d), BF16),
                                pltpu.VMEM((n * cap, ff), BF16), pltpu.VMEM((n, rows, d), BF16),
                                pltpu.VMEM((2, n, rows, d), BF16),
                                dma((4,)), dma((2,)), dma((2,)), dma((2,)), dma, dma((2,)),
                                dma((groups,)), dma((groups,)), dma((groups,)), dma((groups,)),
                                dma((groups,)), dma((groups,)), dma, dma],
                compiler_params=pltpu.CompilerParams(collective_id=1, has_side_effects=True,
                                                     vmem_limit_bytes=67043328),
            )(*operands)[0]

        s_rounds, o_rounds, inner = groups // 2, O_ROUNDS, INNER
        rounds = s_rounds + o_rounds
        scalar = pl.BlockSpec((1, 1), lambda t: (0, 0))
        out, loss, flag, _, _ = pl.pallas_call(
            functools.partial(packed_kernel, n, heads, cap, groups, s_rounds, o_rounds, inner),
            grid=(3 * s_rounds + o_rounds + rounds - inner + s_rounds,),
            out_shape=(jax.ShapeDtypeStruct((groups, seq, d), BF16),
                       jax.ShapeDtypeStruct((1, 1), F32), jax.ShapeDtypeStruct((1, 1), F32),
                       jax.ShapeDtypeStruct((rounds, n * rows, d), BF16),
                       jax.ShapeDtypeStruct((rounds, n * rows, d), BF16)),
            in_specs=group_blocks(lambda t: jnp.minimum(2 * (t // 3) + jnp.minimum(lax.rem(t, 3), 1), last)),
            out_specs=(hbm, scalar, scalar, hbm, hbm),
            scratch_shapes=[pltpu.VMEM((4, d, d), BF16), pltpu.VMEM((3 * experts, d), BF16),
                            pltpu.VMEM((seq, 3 * d), BF16), pltpu.VMEM((seq, d), BF16),
                            pltpu.VMEM((2, 2, seq, d), BF16), pltpu.VMEM((2, seq, d), F32),
                            pltpu.VMEM((groups, 8, seq), F32), pltpu.VMEM((experts, 128), F32),
                            pltpu.VMEM((8, 128), F32), pltpu.VMEM((n, 8, 128), F32),
                            pltpu.VMEM((rounds, n, rows, d), BF16), pltpu.VMEM((groups * seq, d), BF16),
                            pltpu.VMEM((e_loc, d, ff), BF16), pltpu.VMEM((e_loc, ff, d), BF16),
                            dma((4,)), dma((2,)), dma((2,)), dma((2,)), dma((2,)), dma,
                            dma((rounds,)), dma((rounds,)), dma((rounds,)), dma((rounds,)),
                            dma((rounds,)), dma((rounds,)), dma, dma],
            compiler_params=pltpu.CompilerParams(collective_id=0, has_side_effects=True,
                                                 vmem_limit_bytes=67043328),
        )(*operands)
        out = lax.cond(flag[0, 0] > 0.5, full_layer, lambda: out)
        return out, loss[0, 0]

    by_group = P("ep")
    replicated = P()
    placed = (by_group, by_group, by_group, by_group, replicated, replicated, replicated, replicated, replicated, replicated, replicated, by_group, by_group)
    return jax.shard_map(local_step, mesh=mesh, in_specs=placed, out_specs=(by_group, replicated), check_vma=False)
```
